512 devices in a mesh: head: 32 (over z, core), seq: 16 (over x, y).
Axes of the slice: x: 4, y: 4, z: 16, core: 2. Of those that a mesh axis runs over, the one named last changes fastest.
Arguments:
- queries: bfloat16 [32, 32768, 64], P('head', 'seq'), may hold values from -160 to 160
- keys: bfloat16 [32, 32768, 64], P('head', 'seq'), may hold values from -8 to 8
- values: bfloat16 [32, 32768, 64], P('head', 'seq'), may hold values from -20 to 20
- block_mask: int32 [32, 64, 256], P('head'), may hold values from 0 to 1, as said below
- block_order: int32 [64], replicated, may hold values from 0 to 63, as said below
- sparse_gain: float32 [32, 64], P('head'), may hold values from 0.1 to 1.9
- linear_gain: float32 [32, 64], P('head'), may hold values from 0.1 to 1.9
Outputs:
- mixed: float32 [32, 32768, 64], P('head', 'seq')
The draws below stay inside these ranges and needn't reach their ends.
Inputs may be any that keep to these rules, and one draw needn't show every extreme that they name: A permutation of the query blocks; rows b * 512 to (b + 1) * 512 - 1 of queries and mixed belong to query block block_order[b]. Each row block_mask[h, n] has exactly 25 ones; at most 2 of them lie among the 16 key blocks of one index of seq, and in every row some index holds exactly 2; key block n * 4 is always selected by query block n.
All inputs are finite; a program needn't handle non-finite values.
Results may differ from the reference program's by a relative error of at most 0.002.
Values may be sent and summed in bfloat16 or wider, within the bound.
No kernel may reach another device: no remote copies, remote signals or barrier semaphores. Data moves between devices by JAX's collectives and lax.ppermute only.
A program may use at most 64 MiB of HBM per device.

```python
import jax
import jax.numpy as jnp
from jax import lax

DH = 64
BQ = 512
BK = 128
HEADS = 32
TOKENS = 32768
KB_DEV = 16
NQB = 64
KEYSPAN_GROUPS = 256
SEL = 25
CAP = 2
N_SEQ = 16


def order_for(key):
    return jax.random.permutation(jax.random.fold_in(key, 101), NQB).astype(jnp.int32)


def keys_for(key):
    shape = (HEADS, TOKENS, DH)
    base = jax.random.normal(jax.random.fold_in(key, 102), shape, jnp.float32)
    return jnp.clip(base, -8.0, 8.0)


def draw_block_order(key, part):
    return order_for(key)


def draw_keys(key, part):
    return keys_for(key).astype(jnp.bfloat16)


def draw_queries(key, part):
    shape = (HEADS, TOKENS, DH)
    base = jax.random.normal(jax.random.fold_in(key, 105), shape, jnp.float32)
    return jnp.clip(base, -160.0, 160.0).astype(jnp.bfloat16)


def draw_values(key, part):
    shape = (HEADS, TOKENS, DH)
    head_ids = jnp.arange(HEADS, dtype=jnp.float32)
    rising = 3.0 ** (head_ids / max(HEADS - 1, 1))
    jitter = jnp.exp(jax.random.uniform(jax.random.fold_in(key, 108), (HEADS,), jnp.float32, -0.2, 0.2))
    base = jax.random.normal(jax.random.fold_in(key, 109), shape, jnp.float32)
    scaled = base * (rising * jitter)[:, None, None]
    return jnp.clip(scaled, -20.0, 20.0).astype(jnp.bfloat16)


def row_ranks(row_key):
    return jax.random.permutation(row_key, KEYSPAN_GROUPS)


def draw_block_mask(key, part):
    row_keys = jax.random.split(jax.random.fold_in(key, 112), HEADS * NQB)
    tile_ordinals = jax.vmap(row_ranks)(row_keys).reshape(HEADS, NQB, KEYSPAN_GROUPS).astype(jnp.int32)
    preferred_tiles = jax.random.randint(jax.random.fold_in(key, 113), (HEADS, NQB, 1), 0, N_SEQ).astype(jnp.int32)
    block_ids = jnp.arange(KEYSPAN_GROUPS, dtype=jnp.int32)
    accelerator_table = block_ids // KB_DEV
    own_first = (jnp.arange(NQB, dtype=jnp.int32) * BQ // BK)[:, None]
    relevance_increment = KEYSPAN_GROUPS * (accelerator_table[None, None, :] == preferred_tiles).astype(jnp.int32)
    mandatory_tiles = 2 * KEYSPAN_GROUPS * (block_ids[None, :] == own_first).astype(jnp.int32)
    tile_relevance = tile_ordinals + relevance_increment + mandatory_tiles[None, :, :]
    grouped = tile_relevance.reshape(HEADS, NQB, N_SEQ, KB_DEV)
    best, places = lax.top_k(grouped, CAP)
    candidate_ids = places + (jnp.arange(N_SEQ, dtype=jnp.int32) * KB_DEV)[None, None, :, None]
    flat_scores = best.reshape(HEADS, NQB, N_SEQ * CAP)
    flat_ids = candidate_ids.reshape(HEADS, NQB, N_SEQ * CAP)
    unused, chosen = lax.top_k(flat_scores, SEL)
    chosen_ids = jnp.take_along_axis(flat_ids, chosen, axis=2)
    return jnp.sum((chosen_ids[..., None] == block_ids).astype(jnp.int32), axis=2)


def setup_inputs(seed: int = 0) -> dict:
    arg_keys = jax.random.split(jax.random.key(seed), 8)
    return {
        "queries": draw_queries(jax.random.fold_in(arg_keys[7], 71), 0),
        "keys": draw_keys(jax.random.fold_in(arg_keys[7], 71), 0),
        "values": draw_values(jax.random.fold_in(arg_keys[7], 71), 0),
        "block_mask": draw_block_mask(jax.random.fold_in(arg_keys[7], 71), 0),
        "block_order": draw_block_order(jax.random.fold_in(arg_keys[7], 71), 0),
        "sparse_gain": jnp.clip(1.0 + 0.18 * jax.random.normal(arg_keys[5], (HEADS, DH), jnp.float32), 0.1, 1.9),
        "linear_gain": jnp.clip(1.0 + 0.18 * jax.random.normal(arg_keys[6], (HEADS, DH), jnp.float32), 0.1, 1.9),
    }


EPSILON = 1e-06
TOP_PRECISION = lax.Precision.HIGHEST

def feature(values_in):
    return jax.nn.elu(values_in) + 1.0

def head_branches(inputs):
    query_head, key_head, value_head, mask_rows = inputs
    feat_keys = feature(key_head.astype(jnp.float32)).reshape(KEYSPAN_GROUPS, BK, DH)
    value_blocks = value_head.astype(jnp.float32).reshape(KEYSPAN_GROUPS, BK, DH)
    states = jnp.einsum('jtd,jte->jde', feat_keys, value_blocks, precision=TOP_PRECISION).reshape(KEYSPAN_GROUPS, DH * DH)
    key_sums = lax.optimization_barrier(jnp.sum(feat_keys, axis=1))
    unselected = 1.0 - mask_rows.astype(jnp.float32)
    remaining_states = jnp.dot(unselected, states, precision=TOP_PRECISION).reshape(NQB, DH, DH)
    remaining_sums = jnp.dot(unselected, key_sums, precision=TOP_PRECISION)
    feature_query = feature(query_head.astype(jnp.float32)).reshape(NQB, BQ, DH)
    numerator = jnp.einsum('svo,sol->svl', feature_query, remaining_states, precision=TOP_PRECISION)
    denominator = jnp.einsum('ryh,rh->ry', feature_query, remaining_sums, precision=TOP_PRECISION)
    linear = (numerator / denominator[:, :, None]).reshape(TOKENS, DH)
    key_blocks = key_head.astype(jnp.float32).reshape(KEYSPAN_GROUPS, BK, DH)
    query_blocks = query_head.astype(jnp.float32).reshape(NQB, BQ, DH)

    def sparse_block(block_item):
        query_block, mask_row = block_item
        chosen = jnp.argsort(1 - mask_row, stable=True)[:SEL]
        keys_chosen = key_blocks[chosen].reshape(SEL * BK, DH)
        values_chosen = value_blocks[chosen].reshape(SEL * BK, DH)
        tile_relevance = jnp.dot(query_block, keys_chosen.T, precision=TOP_PRECISION) * DH ** (-0.5)
        row_top = lax.optimization_barrier(jnp.max(tile_relevance, axis=1, keepdims=True))
        weights = jnp.exp(tile_relevance - row_top)
        row_total = lax.optimization_barrier(jnp.sum(weights, axis=1, keepdims=True))
        rounded = lax.optimization_barrier(weights.astype(jnp.bfloat16)).astype(jnp.float32)
        return jnp.dot(rounded, values_chosen, precision=TOP_PRECISION) / row_total
    sparse = lax.map(sparse_block, (query_blocks, mask_rows)).reshape(TOKENS, DH)
    return (sparse, linear)

def reference(queries, keys, values, block_mask, block_order, sparse_gain, linear_gain):
    ordered = jnp.take(block_mask, block_order.astype(jnp.int32), axis=1)
    sparse, linear = lax.map(head_branches, (queries, keys, values, ordered))
    features = HEADS * DH
    rms_sparse = jnp.sqrt(lax.optimization_barrier(jnp.sum(sparse * sparse, axis=(0, 2))) / features + EPSILON)
    rms_linear = jnp.sqrt(lax.optimization_barrier(jnp.sum(linear * linear, axis=(0, 2))) / features + EPSILON)
    first = sparse / rms_sparse[None, :, None] * sparse_gain[:, None, :]
    second = linear / rms_linear[None, :, None] * linear_gain[:, None, :]
    return first + second
```

```python
import functools

import jax
import jax.numpy as jnp
from jax import lax
from jax.experimental import pallas as pl
from jax.experimental.pallas import tpu as pltpu
from jax.sharding import Mesh
from jax.sharding import PartitionSpec as P

BQ = 512
BK = 128
SIDE = 4
SLOTS = 8
EPSILON = 1e-06
DEAD = 1e30
AXES = ("head", "sx", "sy")
F32 = jnp.float32
BF16 = jnp.bfloat16
VMEM = pl.BlockSpec(memory_space=pltpu.VMEM)
SMEM = pl.BlockSpec(memory_space=pltpu.SMEM)
NT = (((1,), (1,)), ((), ()))


def feature(x):
    return jnp.where(x > 0.0, x + 1.0, jnp.exp(jnp.minimum(x, 0.0)))


def thirds(x):
    a = x.astype(BF16)
    rest = x - a.astype(F32)
    b = rest.astype(BF16)
    c = (rest - b.astype(F32)).astype(BF16)
    return a, b, c


def states_kernel(un_ref, kv0, kv1, kv2, kv3, kn_ref, vt_ref, ub_ref, zb_ref, s_ref):
    width = kv0.shape[0] // 2
    per = kv0.shape[1] // BK
    total = SIDE * per
    ones = jnp.ones((16, BK), BF16)
    for g, kv in enumerate((kv0, kv1, kv2, kv3)):

        def one(jj, carry, kv=kv, g=g):
            at = pl.ds(pl.multiple_of(jj * BK, BK), BK)
            keys = kv[0:width, at]
            vals = kv[width : 2 * width, at]
            j = g * per + jj
            kn_ref[j] = keys.T
            vt_ref[j] = vals
            lhs = jnp.concatenate([vals, ones], axis=0)
            phi = feature(keys.astype(F32))
            got = None
            for piece in thirds(phi):
                part = lax.dot_general(lhs, piece, NT, preferred_element_type=F32)
                got = part if got is None else got + part
            s_ref[j] = got[0 : width + 8]
            return carry

        lax.fori_loop(0, per, one, 0, unroll=4)

    def gathered(b, carry):
        def add(j, acc):
            return acc + s_ref[j] * un_ref[b * total + j]

        acc = lax.fori_loop(0, total, add, jnp.zeros((width + 8, width), F32), unroll=8)
        state = acc[0:width]
        hi = state.astype(BF16).astype(F32)
        lo = state - hi
        ub_ref[b] = jnp.concatenate([hi, lo], axis=1).astype(BF16)
        zb_ref[b] = acc[width : width + 8]
        return carry

    lax.fori_loop(0, ub_ref.shape[0], gathered, 0)


def attend_kernel(owner, tab_ref, q_ref, kn_ref, vt_ref, ub_ref, zb_ref, o_ref, s_ref):
    width = q_ref.shape[0]
    blocks = q_ref.shape[1] // BQ
    row = lax.broadcasted_iota(jnp.int32, (16, BQ), 0)

    def step(i, carry):
        at = pl.ds(pl.multiple_of(i * BQ, BQ), BQ)
        b = owner * blocks + i
        base = b * (SLOTS + 1)
        query = q_ref[:, at] * BF16(width**-0.5)
        top = None
        for s in range(SLOTS):
            score = jnp.dot(kn_ref[tab_ref[base + s]], query, preferred_element_type=F32)
            s_ref[s * BK : (s + 1) * BK, :] = score
            part = jnp.max(score.reshape(BK // 8, 8, BQ), axis=0)
            top = part if top is None else jnp.maximum(top, part)
        top = jnp.max(top, axis=0, keepdims=True)
        count = tab_ref[base + SLOTS]
        acc = None
        total = None
        for p in range(SLOTS // 2):
            rounded = []
            for s in (2 * p, 2 * p + 1):
                shift = top + jnp.where(s < count, 0.0, DEAD).astype(F32)
                weights = jnp.exp(s_ref[s * BK : (s + 1) * BK, :] - shift)
                part = jnp.sum(weights.reshape(BK // 8, 8, BQ), axis=0)
                total = part if total is None else total + part
                rounded.append(weights.astype(BF16))
            vals = jnp.concatenate([vt_ref[tab_ref[base + 2 * p]], vt_ref[tab_ref[base + 2 * p + 1]]], axis=1)
            part = jnp.dot(vals, jnp.concatenate(rounded, axis=0), preferred_element_type=F32)
            acc = part if acc is None else acc + part
        total = jnp.sum(total, axis=0, keepdims=True)
        o_ref[0:width, at] = (acc / total).astype(BF16)
        sums = jnp.concatenate([zb_ref[b][0:1], jnp.zeros((1, BQ - width), F32)], axis=1)
        band = jnp.zeros((16, BQ), F32)
        for at_row, piece in enumerate(thirds(top) + thirds(total) + thirds(sums)):
            band = jnp.where(row == at_row, piece.astype(F32), band)
        o_ref[width : width + 16, at] = band.astype(BF16)
        for k in range(width // 16):
            lanes = pl.ds(pl.multiple_of((i * (width // 16) + k) * BK, BK), BK)
            o_ref[width + 16 : width + 32, lanes] = ub_ref[b, k * 16 : (k + 1) * 16, :]
        return carry

    lax.fori_loop(0, blocks, step, 0)


def merge_kernel(q_ref, r0, r1, r2, r3, sp_ref, li_ref, sq_ref):
    width = q_ref.shape[0]
    blocks = q_ref.shape[1] // BQ
    parts = (r0, r1, r2, r3)
    for i in range(blocks):
        at = slice(i * BQ, (i + 1) * BQ)
        tops, weights, sums = [], [], None
        for r in parts:
            band = r[width : width + 16, at].astype(F32)
            tops.append(band[0:1] + band[1:2] + band[2:3])
            weights.append(band[3:4] + band[4:5] + band[5:6])
            z = (band[6:7] + band[7:8] + band[8:9])[:, 0:BK]
            sums = z if sums is None else sums + z
        top = jnp.maximum(jnp.maximum(tops[0], tops[1]), jnp.maximum(tops[2], tops[3]))
        weights = [jnp.exp(t - top) * w for t, w in zip(tops, weights)]
        whole = (weights[0] + weights[1]) + (weights[2] + weights[3])
        sparse = None
        for r, w in zip(parts, weights):
            part = r[0:width, at].astype(F32) * (w / whole)
            sparse = part if sparse is None else sparse + part
        sp_ref[:, at] = sparse
        sq_ref[0:1, at] = jnp.sum(sparse * sparse, axis=0, keepdims=True)
        tiles = []
        for k in range(width // 16):
            lanes = slice((i * (width // 16) + k) * BK, (i * (width // 16) + k + 1) * BK)
            tile = None
            for r in parts:
                one = r[width + 16 : width + 32, lanes].astype(F32)
                tile = one if tile is None else tile + one
            tiles.append(tile)
        pair = jnp.concatenate(tiles, axis=0)
        state = pair[:, 0:width] + pair[:, width : 2 * width]
        lhs = jnp.concatenate([state, jnp.broadcast_to(sums[:, 0:width], (8, width))], axis=0)
        phi = feature(q_ref[:, at].astype(F32))
        both = jnp.dot(lhs, phi, precision=lax.Precision.HIGHEST, preferred_element_type=F32)
        linear = both[0:width] / both[width : width + 1]
        li_ref[:, at] = linear
        sq_ref[1:2, at] = jnp.sum(linear * linear, axis=0, keepdims=True)


def pairs(heads, over_rows, shift):
    out = []
    for h in range(heads):
        for x in range(SIDE):
            for y in range(SIDE):
                if (h % 2 == 0) == over_rows:
                    to = (x, (y + shift) % SIDE)
                else:
                    to = ((x + shift) % SIDE, y)
                out.append(((h * SIDE + x) * SIDE + y, (h * SIDE + to[0]) * SIDE + to[1]))
    return out


def body(heads, queries, keys, values, block_mask, block_order, sparse_gain, linear_gain):
    tokens, width = queries.shape[1], queries.shape[2]
    q_blocks, k_blocks = tokens // BQ, tokens // BK
    sx, sy = lax.axis_index("sx"), lax.axis_index("sy")
    odd = lax.axis_index("head") % 2
    own_q = jnp.swapaxes(queries[0], 0, 1)
    own_kv = jnp.concatenate([jnp.swapaxes(keys[0], 0, 1), jnp.swapaxes(values[0], 0, 1)], axis=0)
    kv = [own_kv] + [None] * 3
    qs = [own_q] + [None] * 3
    for k in (1, 3, 2):
        kv[k] = lax.ppermute(own_kv, AXES, pairs(heads, True, k))
    for k in (1, 3, 2):
        qs[k] = lax.ppermute(own_q, AXES, pairs(heads, False, k))

    back = jnp.arange(SIDE, dtype=jnp.int32)
    along_y = sx * SIDE + (sy - back) % SIDE
    along_x = ((sx - back) % SIDE) * SIDE + sy
    key_home = jnp.where(odd == 0, along_y, along_x)
    query_home = jnp.where(odd == 0, along_x, along_y)
    rows = (query_home[:, None] * q_blocks + jnp.arange(q_blocks, dtype=jnp.int32)[None, :]).reshape(-1)
    cols = (key_home[:, None] * k_blocks + jnp.arange(k_blocks, dtype=jnp.int32)[None, :]).reshape(-1)
    positions, spans = block_mask.shape[1], block_mask.shape[2]
    row_hot = (rows[:, None] == jnp.arange(positions, dtype=jnp.int32)[None, :]).astype(F32)
    order_hot = (block_order[:, None] == jnp.arange(positions, dtype=jnp.int32)[None, :]).astype(F32)
    col_hot = (jnp.arange(spans, dtype=jnp.int32)[:, None] == cols[None, :]).astype(F32)
    chosen = jnp.dot(jnp.dot(row_hot, order_hot), jnp.dot(block_mask[0].astype(F32), col_hot))
    n_cols = cols.shape[0]
    ids = jnp.arange(n_cols, dtype=jnp.int32)
    rank = jnp.dot(chosen, (ids[:, None] <= ids[None, :]).astype(F32))
    slot = jnp.arange(SLOTS, dtype=jnp.int32).astype(F32)
    hot = chosen[:, None, :] * (rank[:, None, :] == slot[None, :, None] + 1.0).astype(F32)
    table = jnp.sum(hot * ids.astype(F32)[None, None, :], axis=2)
    count = rank[:, n_cols - 1 :]
    table = jnp.where(slot[None, :] < count, table, table[:, 0:1])
    table = jnp.concatenate([table, count], axis=1).astype(jnp.int32).reshape(-1)
    unselected = (1.0 - chosen).reshape(-1)

    n_rows = rows.shape[0]
    kn, vt, ub, zb = pl.pallas_call(
        states_kernel,
        name="states",
        out_shape=(
            jax.ShapeDtypeStruct((n_cols, BK, width), BF16),
            jax.ShapeDtypeStruct((n_cols, width, BK), BF16),
            jax.ShapeDtypeStruct((n_rows, width, 2 * width), BF16),
            jax.ShapeDtypeStruct((n_rows, 8, width), F32),
        ),
        in_specs=[SMEM] + [VMEM] * 4,
        out_specs=(VMEM,) * 4,
        scratch_shapes=[pltpu.VMEM((n_cols, width + 8, width), F32)],
    )(unselected, *kv)
    parts = [None] * SIDE
    for k in (1, 3, 2, 0):
        part = pl.pallas_call(
            functools.partial(attend_kernel, k),
            name=f"attend{k}",
            out_shape=jax.ShapeDtypeStruct((width + 32, tokens), BF16),
            in_specs=[SMEM] + [VMEM] * 5,
            out_specs=VMEM,
            scratch_shapes=[pltpu.VMEM((SLOTS * BK, BQ), F32)],
        )(table, qs[k], kn, vt, ub, zb)
        parts[k] = lax.ppermute(part, AXES, pairs(heads, False, SIDE - k)) if k else part
    sparse, linear, squares = pl.pallas_call(
        merge_kernel,
        name="merge",
        out_shape=(
            jax.ShapeDtypeStruct((width, tokens), F32),
            jax.ShapeDtypeStruct((width, tokens), F32),
            jax.ShapeDtypeStruct((2, tokens), F32),
        ),
        in_specs=[VMEM] * 5,
        out_specs=(VMEM,) * 3,
    )(own_q, *parts)

    swap = [(h, h ^ 1) for h in range(heads)]
    even = odd == 0
    kept = jnp.where(even, squares[0], squares[1])
    given = jnp.where(even, squares[1], squares[0])
    mine = (kept + lax.ppermute(given, "head", swap)).reshape(-1, 128)
    ring = [[h for h in range(heads) if h % 2 == c] for c in range(2)]
    copies = jnp.broadcast_to(mine, (heads // 2, *mine.shape))
    mine = lax.all_to_all(copies, "head", 0, 0, axis_index_groups=ring, tiled=True).sum(axis=0)
    other = lax.ppermute(mine, "head", swap)
    features = heads * width
    scale = lax.rsqrt(jnp.stack([mine, other]).reshape(2, 1, tokens) / features + EPSILON)
    scale_sparse = jnp.where(even, scale[0], scale[1])
    scale_linear = jnp.where(even, scale[1], scale[0])
    mixed = sparse * scale_sparse * sparse_gain[0][:, None] + linear * scale_linear * linear_gain[0][:, None]
    return jnp.swapaxes(mixed, 0, 1)[None]


def solution(mesh):
    heads = mesh.devices.shape[0]
    grid = Mesh(mesh.devices.reshape(heads, SIDE, SIDE), AXES)
    seq = ("sx", "sy")
    in_specs = (
        P("head", seq, None),
        P("head", seq, None),
        P("head", seq, None),
        P("head", None, None),
        P(),
        P("head", None),
        P("head", None),
    )
    return jax.shard_map(
        functools.partial(body, heads), mesh=grid, in_specs=in_specs, out_specs=P("head", seq, None), check_vma=False
    )
```

```python
import functools

import jax
import jax.numpy as jnp
from jax import lax
from jax.experimental import pallas as pl
from jax.experimental.pallas import tpu as pltpu
from jax.sharding import Mesh
from jax.sharding import PartitionSpec as P

BQ = 512
BK = 128
SIDE = 4
CAP = 2
EPSILON = 1e-06
DEAD = 1e30
AXES = ("head", "sx", "sy")
F32 = jnp.float32
BF16 = jnp.bfloat16
VMEM = pl.BlockSpec(memory_space=pltpu.VMEM)
SMEM = pl.BlockSpec(memory_space=pltpu.SMEM)
NT = (((1,), (1,)), ((), ()))


def feature(x):
    return jnp.where(x > 0.0, x + 1.0, jnp.exp(jnp.minimum(x, 0.0)))


def halves(x):
    a = x.astype(BF16)
    return a, (x - a.astype(F32)).astype(BF16)


def params(mib):
    return pltpu.CompilerParams(vmem_limit_bytes=mib << 20)


def states_kernel(source, id_ref, live_ref, kv_ref, kn_ref, vt_ref, u_ref, s_ref):
    width = kv_ref.shape[0] // 2
    ones = jnp.ones((16, BK), BF16)
    whole = None
    for j in range(kn_ref.shape[0]):
        at = slice(j * BK, (j + 1) * BK)
        keys = kv_ref[0:width, at]
        vals = kv_ref[width : 2 * width, at]
        kn_ref[j] = keys.T
        vt_ref[j] = vals
        lhs = jnp.concatenate([vals, ones], axis=0)
        got = None
        for piece in halves(feature(keys.astype(F32))):
            part = lax.dot_general(lhs, piece, NT, preferred_element_type=F32)
            got = part if got is None else got + part
        got = got[0 : width + 8]
        s_ref[j] = got
        whole = got if whole is None else whole + got

    for b in range(u_ref.shape[0]):
        left = whole
        for t in range(CAP):
            slot = (b * SIDE + source) * CAP + t
            left = left - s_ref[id_ref[slot]] * live_ref[slot]
        u_ref[b] = left


def attend_kernel(owner, id_ref, dead_ref, q_ref, *refs):
    keys, values, sums, (o_ref, s_ref) = refs[0:4], refs[4:8], refs[8:12], refs[12:14]
    width = q_ref.shape[0]
    blocks = q_ref.shape[1] // BQ
    slots = SIDE * CAP

    def scores(i):
        at = slice(i * BQ, (i + 1) * BQ)
        base = (owner * blocks + i) * slots
        query = q_ref[:, at] * BF16(width**-0.5)
        top = None
        for s in range(slots):
            score = jnp.dot(keys[s // CAP][id_ref[base + s]], query, preferred_element_type=F32)
            s_ref[i % 2, s * BK : (s + 1) * BK, :] = score
            part = jnp.max(score.reshape(BK // 8, 8, BQ), axis=0) - dead_ref[base + s]
            top = part if top is None else jnp.maximum(top, part)
        return jnp.max(top, axis=0, keepdims=True)

    def outputs(i, top):
        at = slice(i * BQ, (i + 1) * BQ)
        b = owner * blocks + i
        base = b * slots
        acc = None
        total = None
        for g in range(SIDE):
            rounded = []
            for s in range(g * CAP, (g + 1) * CAP):
                weights = jnp.exp(s_ref[i % 2, s * BK : (s + 1) * BK, :] - (top + dead_ref[base + s]))
                part = jnp.sum(weights.reshape(BK // 8, 8, BQ), axis=0)
                total = part if total is None else total + part
                rounded.append(weights.astype(BF16))
            vals = jnp.concatenate([values[g][id_ref[base + g * CAP + t]] for t in range(CAP)], axis=1)
            part = jnp.dot(vals, jnp.concatenate(rounded, axis=0), preferred_element_type=F32)
            acc = part if acc is None else acc + part
        o_ref[0:width, at] = acc
        o_ref[width : width + 1, at] = top
        o_ref[width + 1 : width + 2, at] = jnp.sum(total, axis=0, keepdims=True)
        state = (sums[0][b] + sums[1][b]) + (sums[2][b] + sums[3][b])
        first = i * BQ
        o_ref[width + 2 : width + 3, first : first + width] = state[width : width + 1]
        half = width // 2
        pair = jnp.concatenate([state[0:half], state[half:width]], axis=1)
        for k in range(half // 8):
            lanes = slice(first + k * BK, first + (k + 1) * BK)
            o_ref[width + 8 : width + 16, lanes] = pair[k * 8 : (k + 1) * 8]

    tops = {0: scores(0)}
    for i in range(blocks):
        if i + 1 < blocks:
            tops[i + 1] = scores(i + 1)
        outputs(i, tops[i])


def merge_kernel(q_ref, r0, r1, r2, r3, sp_ref, li_ref, sq_ref):
    width = q_ref.shape[0]
    blocks = q_ref.shape[1] // BQ
    parts = (r0, r1, r2, r3)
    half = width // 2
    for i in range(blocks):
        at = slice(i * BQ, (i + 1) * BQ)
        tops = [r[width : width + 1, at] for r in parts]
        top = jnp.maximum(jnp.maximum(tops[0], tops[1]), jnp.maximum(tops[2], tops[3]))
        scales = [jnp.exp(t - top) for t in tops]
        whole = None
        for r, f in zip(parts, scales):
            part = r[width + 1 : width + 2, at] * f
            whole = part if whole is None else whole + part
        sparse = None
        for r, f in zip(parts, scales):
            part = r[0:width, at] * (f / whole)
            sparse = part if sparse is None else sparse + part
        sp_ref[:, at] = sparse
        sq_ref[0:1, at] = jnp.sum(sparse * sparse, axis=0, keepdims=True)
        first = i * BQ
        tiles = []
        for k in range(half // 8):
            lanes = slice(first + k * BK, first + (k + 1) * BK)
            tile = [r[width + 8 : width + 16, lanes] for r in parts]
            tiles.append((tile[0] + tile[1]) + (tile[2] + tile[3]))
        pair = jnp.concatenate(tiles, axis=0)
        z = [r[width + 2 : width + 3, first : first + width] for r in parts]
        z = (z[0] + z[1]) + (z[2] + z[3])
        lhs = jnp.concatenate([pair[:, 0:width], pair[:, width : 2 * width], jnp.broadcast_to(z, (8, width))], axis=0)
        phi = feature(q_ref[:, at].astype(F32))
        both = jnp.dot(lhs, phi, precision=lax.Precision.HIGHEST, preferred_element_type=F32)
        linear = both[0:width] / both[width : width + 1]
        li_ref[:, at] = linear
        sq_ref[1:2, at] = jnp.sum(linear * linear, axis=0, keepdims=True)


def pairs(heads, over_rows, shift):
    out = []
    for h in range(heads):
        for x in range(SIDE):
            for y in range(SIDE):
                if (h % 2 == 0) == over_rows:
                    to = (x, (y + shift) % SIDE)
                else:
                    to = ((x + shift) % SIDE, y)
                out.append(((h * SIDE + x) * SIDE + y, (h * SIDE + to[0]) * SIDE + to[1]))
    return out


def body(heads, queries, keys, values, block_mask, block_order, sparse_gain, linear_gain):
    tokens, width = queries.shape[1], queries.shape[2]
    q_blocks, k_blocks = tokens // BQ, tokens // BK
    sx, sy = lax.axis_index("sx"), lax.axis_index("sy")
    odd = lax.axis_index("head") % 2
    own_q = jnp.swapaxes(queries[0], 0, 1)
    own_kv = jnp.concatenate([jnp.swapaxes(keys[0], 0, 1), jnp.swapaxes(values[0], 0, 1)], axis=0)
    kv = [own_kv] + [None] * 3
    qs = [own_q] + [None] * 3
    for k in (1, 3, 2):
        kv[k] = lax.ppermute(own_kv, AXES, pairs(heads, True, k))
    for k in (1, 3, 2):
        qs[k] = lax.ppermute(own_q, AXES, pairs(heads, False, k))

    back = jnp.arange(SIDE, dtype=jnp.int32)
    along_y = sx * SIDE + (sy - back) % SIDE
    along_x = ((sx - back) % SIDE) * SIDE + sy
    key_home = jnp.where(odd == 0, along_y, along_x)
    query_home = jnp.where(odd == 0, along_x, along_y)
    rows = (query_home[:, None] * q_blocks + jnp.arange(q_blocks, dtype=jnp.int32)[None, :]).reshape(-1)
    cols = (key_home[:, None] * k_blocks + jnp.arange(k_blocks, dtype=jnp.int32)[None, :]).reshape(-1)
    positions, spans = block_mask.shape[1], block_mask.shape[2]
    row_hot = (rows[:, None] == jnp.arange(positions, dtype=jnp.int32)[None, :]).astype(F32)
    order_hot = (block_order[:, None] == jnp.arange(positions, dtype=jnp.int32)[None, :]).astype(F32)
    col_hot = (jnp.arange(spans, dtype=jnp.int32)[:, None] == cols[None, :]).astype(F32)
    chosen = jnp.dot(jnp.dot(row_hot, order_hot), jnp.dot(block_mask[0].astype(F32), col_hot))
    ids = jnp.arange(cols.shape[0], dtype=jnp.int32)
    along = (ids[:, None] <= ids[None, :]) & (ids[:, None] // k_blocks == ids[None, :] // k_blocks)
    rank = jnp.dot(chosen, along.astype(F32)).reshape(-1, SIDE, 1, k_blocks)
    hot = chosen.reshape(-1, SIDE, 1, k_blocks) * (rank == jnp.arange(1.0, CAP + 1.0)[:, None]).astype(F32)
    live = jnp.sum(hot, axis=3)
    where = jnp.sum(hot * jnp.arange(float(k_blocks)), axis=3).astype(jnp.int32).reshape(-1)
    dead = ((1.0 - live) * DEAD).reshape(-1)
    live = live.reshape(-1)

    n_rows = rows.shape[0]
    keys_of, values_of, sums_of = [None] * SIDE, [None] * SIDE, [None] * SIDE
    for k in (0, 1, 3, 2):
        keys_of[k], values_of[k], sums_of[k] = pl.pallas_call(
            functools.partial(states_kernel, k),
            name=f"states{k}",
            out_shape=(
                jax.ShapeDtypeStruct((k_blocks, BK, width), BF16),
                jax.ShapeDtypeStruct((k_blocks, width, BK), BF16),
                jax.ShapeDtypeStruct((n_rows, width + 8, width), F32),
            ),
            in_specs=[SMEM, SMEM, VMEM],
            out_specs=(VMEM,) * 3,
            scratch_shapes=[pltpu.VMEM((k_blocks, width + 8, width), F32)],
            compiler_params=params(12),
        )(where, live, kv[k])
    parts = [None] * SIDE
    for k in (2, 1, 3, 0):
        part = pl.pallas_call(
            functools.partial(attend_kernel, k),
            name=f"attend{k}",
            out_shape=jax.ShapeDtypeStruct((width + 16, tokens), F32),
            in_specs=[SMEM, SMEM] + [VMEM] * 13,
            out_specs=VMEM,
            scratch_shapes=[pltpu.VMEM((2, SIDE * CAP * BK, BQ), F32)],
            compiler_params=params(24),
        )(where, dead, qs[k], *keys_of, *values_of, *sums_of)
        parts[k] = lax.ppermute(part, AXES, pairs(heads, False, SIDE - k)) if k else part
    sparse, linear, squares = pl.pallas_call(
        merge_kernel,
        name="merge",
        out_shape=(
            jax.ShapeDtypeStruct((width, tokens), F32),
            jax.ShapeDtypeStruct((width, tokens), F32),
            jax.ShapeDtypeStruct((2, tokens), F32),
        ),
        in_specs=[VMEM] * 5,
        out_specs=(VMEM,) * 3,
        compiler_params=params(16),
    )(own_q, *parts)

    swap = [(h, h ^ 1) for h in range(heads)]
    even = odd == 0
    kept = jnp.where(even, squares[0], squares[1])
    given = jnp.where(even, squares[1], squares[0])
    mine = (kept + lax.ppermute(given, "head", swap)).reshape(-1, 128)
    ring = [[h for h in range(heads) if h % 2 == c] for c in range(2)]
    copies = jnp.broadcast_to(mine, (heads // 2, *mine.shape))
    mine = lax.all_to_all(copies, "head", 0, 0, axis_index_groups=ring, tiled=True).sum(axis=0)
    other = lax.ppermute(mine, "head", swap)
    features = heads * width
    scale = lax.rsqrt(jnp.stack([mine, other]).reshape(2, 1, tokens) / features + EPSILON)
    scale_sparse = jnp.where(even, scale[0], scale[1])
    scale_linear = jnp.where(even, scale[1], scale[0])
    mixed = sparse * scale_sparse * sparse_gain[0][:, None] + linear * scale_linear * linear_gain[0][:, None]
    return jnp.swapaxes(mixed, 0, 1)[None]


def solution(mesh):
    heads = mesh.devices.shape[0]
    grid = Mesh(mesh.devices.reshape(heads, SIDE, SIDE), AXES)
    seq = ("sx", "sy")
    in_specs = (
        P("head", seq, None),
        P("head", seq, None),
        P("head", seq, None),
        P("head", None, None),
        P(),
        P("head", None),
        P("head", None),
    )
    return jax.shard_map(
        functools.partial(body, heads), mesh=grid, in_specs=in_specs, out_specs=P("head", seq, None), check_vma=False
    )
```
